32 devices in a mesh: dp: 1 (over z), tp: 4 (over y), cp: 8 (over x, core).
Axes of the slice: x: 4, y: 4, z: 1, core: 2. Of those that a mesh axis runs over, the one named last changes fastest.
The devices are a block of a 4x4x8 slice.
Arguments:
- hidden: bfloat16 [16, 64, 5120], P('dp')
- attn_gain: bfloat16 [5120], replicated
- w_query: bfloat16 [5120, 4096], P(None, 'tp')
- w_key: bfloat16 [5120, 1024], P(None, 'tp')
- w_value: bfloat16 [5120, 1024], P(None, 'tp')
- w_out: bfloat16 [4096, 5120], P('tp')
- cache_k: bfloat16 [16, 4, 8, 8, 256, 128], P('dp', None, 'cp', 'tp')
- cache_v: bfloat16 [16, 4, 8, 8, 256, 128], P('dp', None, 'cp', 'tp')
- ctx_len: int32 [16], P('dp')
- positions: int32 [16, 64], P('dp')
- tree_mask: int32 [16, 64, 64], P('dp')
Outputs:
- output 1: bfloat16 [16, 64, 5120], P('dp')
- output 2: bfloat16 [16, 4, 8, 8, 256, 128], P('dp', None, 'cp', 'tp')
- output 3: bfloat16 [16, 4, 8, 8, 256, 128], P('dp', None, 'cp', 'tp')
All inputs are finite; a program needn't handle non-finite values.
Results may differ from the reference program's by a relative error of at most 0.0082716.
Values sent between devices are 32-bit elements.
A program may use at most 768 MiB of HBM per device.

```python
import math
import jax
import jax.numpy as jnp
from jax import lax

D = 5120
HEADS = 32
KV_HEADS = 8
HEAD = 128
REQ = 16
TREE = 64
BLOCKS_DEV = 4
CP = 8
TP = 4
BLOCK = 256
ROPE_THETA = 500000.0
NORM_EPS = 1e-5
MASKED = -1e30


def rope_tables(positions, head_dim):
    freq_idx = jnp.arange(head_dim // 2, dtype=jnp.float32)
    inv_freq = 1.0 / (ROPE_THETA ** (2.0 * freq_idx / head_dim))
    wavelen = 2.0 * math.pi / inv_freq
    smooth = (8192.0 / wavelen - 1.0) / 3.0
    blended = (1.0 - smooth) * inv_freq / 8.0 + smooth * inv_freq
    inv_freq = jnp.where(wavelen < 2048.0, inv_freq, jnp.where(wavelen > 8192.0, inv_freq / 8.0, blended))
    angle = positions.astype(jnp.float32)[..., None] * inv_freq
    return jnp.cos(angle)[..., None, :], jnp.sin(angle)[..., None, :]


def apply_rope(values, cos_tab, sin_tab):
    half = values.shape[-1] // 2
    first = values[..., :half]
    second = values[..., half:]
    return jnp.concatenate([first * cos_tab - second * sin_tab, second * cos_tab + first * sin_tab], axis=-1)


def rms_norm(hidden, attn_gain):
    wide = hidden.astype(jnp.float32)
    inv_rms = lax.rsqrt(jnp.mean(wide * wide, axis=-1, keepdims=True) + NORM_EPS)
    return wide, (wide * inv_rms * attn_gain.astype(jnp.float32)).astype(jnp.bfloat16)


def draw_structure(key):
    ctx_key, tree_key = jax.random.split(key)
    max_len = BLOCKS_DEV * CP * BLOCK
    ctx_len = jax.random.randint(ctx_key, (REQ,), max_len // 2, max_len - TREE + 1, dtype=jnp.int32)
    ctx_len = ctx_len.at[0].set(max_len - TREE).at[1].set(max_len // 2)
    raw = jax.random.randint(tree_key, (REQ, TREE), 0, 1 << 30, dtype=jnp.int32)
    node_ids = jnp.arange(TREE, dtype=jnp.int32)
    parents = raw % jnp.maximum(node_ids, 1)[None, :]
    ancestry = jnp.broadcast_to(jnp.eye(TREE, dtype=jnp.int32), (REQ, TREE, TREE))
    for node in range(1, TREE):
        above = jnp.take_along_axis(ancestry, parents[:, node][:, None, None], axis=1)[:, 0, :]
        ancestry = ancestry.at[:, node, :].add(above)
    depth = ancestry.sum(axis=-1) - 1
    positions = ctx_len[:, None] + depth
    return ctx_len, positions.astype(jnp.int32), ancestry


def setup_inputs(seed: int = 0, part: int = 0) -> dict:
    base = jax.random.key(seed)
    part_key = jax.random.fold_in(base, part)
    wkeys = jax.random.split(base, 5)
    pkeys = jax.random.split(part_key, 4)
    max_len = BLOCKS_DEV * CP * BLOCK
    key_scale = math.sqrt(math.log(max_len / 64.0))
    new_scale = math.log(max_len) - 1.4
    ctx_len, positions, tree_mask = draw_structure(pkeys[0])
    hidden = (0.5 * jax.random.normal(pkeys[1], (REQ, TREE, D), jnp.float32)).astype(jnp.bfloat16)
    attn_gain = (1.0 + 0.3 * jax.random.normal(wkeys[0], (D,), jnp.float32)).astype(jnp.bfloat16)
    w_query = (jax.random.normal(wkeys[1], (D, HEADS * HEAD), jnp.float32) * D ** -0.5).astype(jnp.bfloat16)
    w_key = (jax.random.normal(wkeys[2], (D, KV_HEADS * HEAD), jnp.float32) * (new_scale * D ** -0.5)).astype(jnp.bfloat16)
    w_value = (jax.random.normal(wkeys[3], (D, KV_HEADS * HEAD), jnp.float32) * (2.0 * D ** -0.5)).astype(jnp.bfloat16)
    w_out = (jax.random.normal(wkeys[4], (HEADS * HEAD, D), jnp.float32) * (HEADS * HEAD) ** -0.5).astype(jnp.bfloat16)
    cache_shape = (REQ, BLOCKS_DEV, CP, KV_HEADS, BLOCK, HEAD)
    cache_k = (key_scale * jax.random.normal(pkeys[2], cache_shape, jnp.float32)).astype(jnp.bfloat16)
    cache_v = (4.0 * jax.random.normal(pkeys[3], cache_shape, jnp.float32)).astype(jnp.bfloat16)
    return {'hidden': hidden, 'attn_gain': attn_gain, 'w_query': w_query, 'w_key': w_key, 'w_value': w_value, 'w_out': w_out, 'cache_k': cache_k, 'cache_v': cache_v, 'ctx_len': ctx_len, 'positions': positions, 'tree_mask': tree_mask}


def reference(hidden, attn_gain, w_query, w_key, w_value, w_out, cache_k, cache_v, ctx_len, positions, tree_mask):
    group = HEADS // KV_HEADS
    max_len = BLOCKS_DEV * CP * BLOCK
    scale = HEAD ** -0.5
    wide, normed = rms_norm(hidden, attn_gain)
    flat_rows = normed.reshape(REQ * TREE, D)
    query = jnp.dot(flat_rows, w_query, preferred_element_type=jnp.float32).reshape(REQ, TREE, HEADS, HEAD)
    key_new = jnp.dot(flat_rows, w_key, preferred_element_type=jnp.float32).reshape(REQ, TREE, KV_HEADS, HEAD)
    val_new = jnp.dot(flat_rows, w_value, preferred_element_type=jnp.float32).astype(jnp.bfloat16).reshape(REQ, TREE, KV_HEADS, HEAD)
    cos_tab, sin_tab = rope_tables(positions, HEAD)
    query = apply_rope(query, cos_tab, sin_tab).astype(jnp.bfloat16)
    key_new = apply_rope(key_new, cos_tab, sin_tab).astype(jnp.bfloat16)

    def attend_one(item):
        q_one, key_one, val_one, cache_k_one, cache_v_one, ctx_one, mask_one = item
        keys_all = jnp.transpose(cache_k_one, (0, 1, 3, 2, 4)).reshape(max_len, KV_HEADS, HEAD).astype(jnp.float32)
        vals_all = jnp.transpose(cache_v_one, (0, 1, 3, 2, 4)).reshape(max_len, KV_HEADS, HEAD).astype(jnp.float32)
        q_wide = q_one.reshape(TREE, KV_HEADS, group, HEAD).astype(jnp.float32)
        score_cache = jnp.einsum('tkgd,lkd->tkgl', q_wide, keys_all) * scale
        valid = jnp.arange(max_len) < ctx_one
        score_cache = jnp.where(valid, score_cache, MASKED)
        score_tree = jnp.einsum('tkgd,skd->tkgs', q_wide, key_one.astype(jnp.float32)) * scale
        tree_ok = (mask_one > 0)[:, None, None, :]
        score_tree = jnp.where(tree_ok, score_tree, MASKED)
        row_max = jnp.maximum(score_cache.max(axis=-1), score_tree.max(axis=-1))
        prob_cache = jnp.exp(score_cache - row_max[..., None])
        prob_tree = jnp.exp(score_tree - row_max[..., None])
        row_sum = prob_cache.sum(axis=-1) + prob_tree.sum(axis=-1)
        mixed = jnp.einsum('tkgl,lkd->tkgd', prob_cache, vals_all) + jnp.einsum('tkgs,skd->tkgd', prob_tree, val_one.astype(jnp.float32))
        return (mixed / row_sum[..., None]).reshape(TREE, HEADS * HEAD).astype(jnp.bfloat16)

    attn = lax.map(attend_one, (query, key_new, val_new, cache_k, cache_v, ctx_len, tree_mask))
    head_part = HEADS * HEAD // TP
    grouped = attn.reshape(REQ, TREE, TP, head_part).astype(jnp.float32)
    proj = jnp.einsum('rtgf,gfe->rtge', grouped, w_out.reshape(TP, head_part, D).astype(jnp.float32)).astype(jnp.bfloat16)
    out_hidden = (wide + proj.astype(jnp.float32).sum(axis=2)).astype(jnp.bfloat16)
    slot_ids = ctx_len[:, None] + jnp.arange(TREE)[None, :]
    block_ids = slot_ids // BLOCK
    req_ids = jnp.broadcast_to(jnp.arange(REQ)[:, None], (REQ, TREE))
    new_cache_k = cache_k.at[req_ids, block_ids // CP, block_ids % CP, :, slot_ids % BLOCK, :].set(key_new)
    new_cache_v = cache_v.at[req_ids, block_ids // CP, block_ids % CP, :, slot_ids % BLOCK, :].set(val_new)
    return (out_hidden, new_cache_k, new_cache_v)
```

```python
import functools
import math

import jax
import jax.numpy as jnp
from jax import lax
from jax.experimental import pallas as pl
from jax.experimental.pallas import tpu as pltpu
from jax.sharding import PartitionSpec as P

MESH = pl.DeviceIdType.MESH
ROPE_THETA = 500000.0
NORM_EPS = 1e-5
MASKED = -1e30
NUM_CHUNKS = 2
STAT_ROWS = 8
F32 = jnp.float32
BF16 = jnp.bfloat16


def rope_tables(positions, head_dim):
    freq_idx = jnp.arange(head_dim // 2, dtype=F32)
    inv_freq = 1.0 / (ROPE_THETA ** (2.0 * freq_idx / head_dim))
    wavelen = 2.0 * math.pi / inv_freq
    smooth = (8192.0 / wavelen - 1.0) / 3.0
    blended = (1.0 - smooth) * inv_freq / 8.0 + smooth * inv_freq
    inv_freq = jnp.where(wavelen < 2048.0, inv_freq, jnp.where(wavelen > 8192.0, inv_freq / 8.0, blended))
    angle = positions.astype(F32).reshape(-1)[:, None] * inv_freq
    cos_tab, sin_tab = jnp.cos(angle), jnp.sin(angle)
    return jnp.concatenate([cos_tab, cos_tab], axis=-1), jnp.concatenate([-sin_tab, sin_tab], axis=-1)


def qkv_kernel(x_ref, gain_ref, cos_ref, sin_ref, wq_ref, wk_ref, wv_ref, q_ref, k_ref, v_ref):
    head_dim = cos_ref.shape[1]
    wide = x_ref[...].astype(F32)
    inv_rms = lax.rsqrt(jnp.mean(wide * wide, axis=-1, keepdims=True) + NORM_EPS)
    normed = (wide * inv_rms * gain_ref[...].astype(F32)).astype(BF16)
    cos_tab, sin_tab = cos_ref[...], sin_ref[...]

    def rotate(full, out_ref):
        for h in range(full.shape[1] // head_dim):
            part = full[:, h * head_dim:(h + 1) * head_dim]
            out_ref[:, h * head_dim:(h + 1) * head_dim] = (part * cos_tab + pltpu.roll(part, head_dim // 2, 1) * sin_tab).astype(BF16)

    rotate(jnp.dot(normed, wq_ref[...], preferred_element_type=F32), q_ref)
    rotate(jnp.dot(normed, wk_ref[...], preferred_element_type=F32), k_ref)
    v_ref[...] = jnp.dot(normed, wv_ref[...], preferred_element_type=F32).astype(BF16)


def project_qkv(x_rows, gain, cos_tab, sin_tab, wq, wk, wv):
    rows, width = x_rows.shape
    tile = min(128, rows)
    row_block = lambda n: pl.BlockSpec((tile, n), lambda i: (i, 0))
    whole = lambda a: pl.BlockSpec(a.shape, lambda i: (0, 0), pipeline_mode=pl.Buffered(1))
    return pl.pallas_call(
        qkv_kernel,
        grid=(rows // tile,),
        in_specs=[row_block(width), whole(gain), row_block(cos_tab.shape[1]), row_block(cos_tab.shape[1]), whole(wq), whole(wk), whole(wv)],
        out_specs=[row_block(wq.shape[1]), row_block(wk.shape[1]), row_block(wv.shape[1])],
        out_shape=[jax.ShapeDtypeStruct((rows, w.shape[1]), BF16) for w in (wq, wk, wv)],
        compiler_params=pltpu.CompilerParams(dimension_semantics=("arbitrary",)),
        name="qkv",
    )(x_rows, gain, cos_tab, sin_tab, wq, wk, wv)


def attn_kernel(cp_size, halves, ctx_ref, cp_ref, q_ref, kn_ref, vn_ref, mask_ref, kc_ref, vc_ref, a_ref, nk_ref, nv_ref):
    num_blocks, kv_local, blk_len, head_dim = kc_ref.shape
    tree_len = q_ref.shape[0]
    group = q_ref.shape[1] // (kv_local * head_dim)
    sub = tree_len // halves
    lanes = group * tree_len
    ctx = ctx_ref[pl.program_id(0)]
    cp_rank = cp_ref[0]
    scale = head_dim ** -0.5 * math.log2(math.e)
    nk_ref[...] = kc_ref[...]
    nv_ref[...] = vc_ref[...]
    mask = mask_ref[...].astype(F32)
    mask_rows = jnp.concatenate([mask[hf * sub:(hf + 1) * sub] for hf in range(halves) for _ in range(group)], axis=0)
    tree_ok = (mask_rows.T > 0) & (cp_rank == 0)
    for kv in range(kv_local):
        q_rows = jnp.concatenate(
            [q_ref[hf * sub:(hf + 1) * sub, (kv * group + g) * head_dim:(kv * group + g + 1) * head_dim] for hf in range(halves) for g in range(group)], axis=0)
        kn = kn_ref[:, kv * head_dim:(kv + 1) * head_dim]
        vn = vn_ref[:, kv * head_dim:(kv + 1) * head_dim]
        nt = (((1,), (1,)), ((), ()))
        tn = (((0,), (0,)), ((), ()))
        scores = []
        for j in range(num_blocks):
            s = lax.dot_general(kc_ref[j, kv], q_rows, nt, preferred_element_type=F32)
            if j >= num_blocks // 2:
                pos = (j * cp_size + cp_rank) * blk_len + lax.broadcasted_iota(jnp.int32, s.shape, 0)
                s = jnp.where(pos < ctx, s, MASKED)
            scores.append(s)
        s = lax.dot_general(kn, q_rows, nt, preferred_element_type=F32)
        scores.append(jnp.where(tree_ok, s, MASKED))
        row_max = functools.reduce(jnp.maximum, [s.max(axis=0, keepdims=True) for s in scores])
        row_sum, out = 0.0, 0.0
        for j, s in enumerate(scores):
            p = jnp.exp2((s - row_max) * scale)
            row_sum = row_sum + p.sum(axis=0, keepdims=True)
            vals = vc_ref[j, kv] if j < num_blocks else vn
            out = out + lax.dot_general(vals, p.astype(BF16), tn, preferred_element_type=F32)
        stat = jnp.where(lax.broadcasted_iota(jnp.int32, (STAT_ROWS, lanes), 0) < STAT_ROWS // 2, row_max, row_sum)
        width = lanes // halves
        for hf in range(halves):
            a_ref[hf, kv, :head_dim] = out[:, hf * width:(hf + 1) * width]
            a_ref[hf, kv, head_dim:] = stat[:, hf * width:(hf + 1) * width]
    first = ctx // blk_len
    for extra in range(2):
        blk = first + extra
        loc = blk // cp_size

        @pl.when((blk % cp_size == cp_rank) & (loc < num_blocks))
        def _():
            source = lax.broadcasted_iota(jnp.int32, (blk_len, tree_len), 0) + (blk * blk_len - ctx)
            pick = (source == lax.broadcasted_iota(jnp.int32, (blk_len, tree_len), 1)).astype(BF16)
            at = lax.broadcasted_iota(jnp.int32, (blk_len, head_dim), 0) + (blk * blk_len - ctx)
            inside = (at >= 0) & (at < tree_len)
            for kv in range(kv_local):
                for new_ref, old_ref, out_ref in ((kn_ref, kc_ref, nk_ref), (vn_ref, vc_ref, nv_ref)):
                    moved = jnp.dot(pick, new_ref[:, kv * head_dim:(kv + 1) * head_dim], preferred_element_type=F32)
                    out_ref[loc, kv] = jnp.where(inside, moved, old_ref[loc, kv].astype(F32)).astype(BF16)


def attend(cp_size, halves, ctx_len, cp_rank, q, kn, vn, tree_mask, cache_k, cache_v):
    num_reqs, num_blocks, _, kv_local, blk_len, head_dim = cache_k.shape
    tree_len = tree_mask.shape[1]
    group = q.shape[1] // (kv_local * head_dim)
    lanes = group * tree_len // halves
    rows = lambda a: pl.BlockSpec((tree_len, a.shape[1]), lambda i, *_: (i, 0))
    cache = pl.BlockSpec((None, num_blocks, None, kv_local, blk_len, head_dim), lambda i, *_: (i, 0, 0, 0, 0, 0))
    a_shape = (num_reqs, halves, kv_local, head_dim + STAT_ROWS, lanes)
    return pl.pallas_call(
        functools.partial(attn_kernel, cp_size, halves),
        grid_spec=pltpu.PrefetchScalarGridSpec(
            num_scalar_prefetch=2, grid=(num_reqs,),
            in_specs=[rows(q), rows(kn), rows(vn), pl.BlockSpec((None, tree_len, tree_len), lambda i, *_: (i, 0, 0)), cache, cache],
            out_specs=[pl.BlockSpec((None,) + a_shape[1:], lambda i, *_: (i, 0, 0, 0, 0)), cache, cache]),
        out_shape=[jax.ShapeDtypeStruct(a_shape, F32), jax.ShapeDtypeStruct(cache_k.shape, BF16), jax.ShapeDtypeStruct(cache_v.shape, BF16)],
        compiler_params=pltpu.CompilerParams(dimension_semantics=("arbitrary",)),
        name="attn",
    )(ctx_len, cp_rank, q, kn, vn, tree_mask, cache_k, cache_v)


def combine_kernel(num_chunks, nx, ny, scale, a_ref, hid_ref, w_hbm, y_hbm, w_ref, xres, d2d, step1, step2, heads_ref, part, tp1, tp2, full, stage,
                   w_sem, x_sem, out_sem, rs_send, rs_recv, ag_send, ag_recv, pr_send, pr_recv):
    head_dim = a_ref.shape[4] - STAT_ROWS
    kv_local = a_ref.shape[3]
    lanes = a_ref.shape[5]
    toks = heads_ref.shape[0]
    rows = xres.shape[1]
    width = xres.shape[2]
    group = lanes // toks
    quarter = width // 4
    half = width // 2
    cp = lax.axis_index('cp')
    me_x, core = cp // 2, cp % 2
    me_y = lax.axis_index('tp')
    other = 1 - core
    xs = [me_x] + [lax.rem(me_x + d, nx) for d in range(1, nx)]
    ys = [me_y] + [lax.rem(me_y + d, ny) for d in range(1, ny)]
    right = {'cp': xs[1] * 2 + core}
    left = {'cp': xs[3] * 2 + core}
    up = {'tp': ys[1]}
    down = {'tp': ys[3]}
    partner = {'cp': me_x * 2 + other}

    barrier = pltpu.get_barrier_semaphore()
    for peer in (right, left, up, down, partner):
        pl.semaphore_signal(barrier, inc=1, device_id=peer, device_id_type=MESH)
    pl.semaphore_wait(barrier, 5)

    def remote(src, dst, ssem, rsem, peer):
        return pltpu.make_async_remote_copy(src_ref=src, dst_ref=dst, send_sem=ssem, recv_sem=rsem, device_id=peer, device_id_type=MESH)

    w_copy = pltpu.make_async_copy(w_hbm, w_ref, w_sem)
    w_copy.start()
    x_copies = []
    for ch in range(num_chunks):
        block = ((ch * nx + me_x) * 2 + core) * ny + me_y
        copy = pltpu.make_async_copy(hid_ref.at[block], xres.at[ch], x_sem.at[ch])
        copy.start()
        x_copies.append(copy)

    rs = [dict() for _ in range(num_chunks)]
    for ch in range(num_chunks):
        for i, xd in enumerate((2, 1, 3, 0)):
            copy = remote(a_ref.at[ch, xs[xd], other], d2d.at[ch, xs[xd]], rs_send.at[ch, i], rs_recv.at[ch, i], partner)
            copy.start()
            rs[ch]['d', xd] = copy

    def stat_of(ref):
        return ref[head_dim:head_dim + 1], ref[head_dim + STAT_ROWS // 2:head_dim + STAT_ROWS // 2 + 1]

    def merged(refs):
        stats = [stat_of(r) for r in refs]
        top = functools.reduce(jnp.maximum, [m for m, _ in stats])
        factors = [jnp.exp2((m - top) * scale) for m, _ in stats]
        total = sum(l * f for (_, l), f in zip(stats, factors))
        mixed = sum(r[:head_dim] * f for r, f in zip(refs, factors))
        return mixed, top, total

    def merge_into(dst, refs):
        mixed, top, total = merged(refs)
        dst[:head_dim] = mixed
        dst[head_dim:] = jnp.where(lax.broadcasted_iota(jnp.int32, (STAT_ROWS, lanes), 0) < STAT_ROWS // 2, top, total)

    def cp_pair(ch):
        for xd in (2, 1, 3, 0):
            rs[ch]['d', xd].wait_recv()
            for kv in range(kv_local):
                dst = d2d.at[ch, xs[xd], kv]
                merge_into(dst, [a_ref.at[ch, xs[xd], core, kv], dst])
            if xd == 2:
                rs[ch]['r1'] = remote(d2d.at[ch, xs[2], 0], step1.at[ch, 0], rs_send.at[ch, 4], rs_recv.at[ch, 4], right)
                rs[ch]['l1'] = remote(d2d.at[ch, xs[2], 1], step1.at[ch, 1], rs_send.at[ch, 5], rs_recv.at[ch, 5], left)
                rs[ch]['r1'].start()
                rs[ch]['l1'].start()

    def cp_step(ch):
        rs[ch]['r1'].wait_recv()
        dst = d2d.at[ch, xs[1], 0]
        merge_into(dst, [dst, step1.at[ch, 0]])
        rs[ch]['r2'] = remote(d2d.at[ch, xs[1]], step2.at[ch, 0], rs_send.at[ch, 6], rs_recv.at[ch, 6], right)
        rs[ch]['r2'].start()
        rs[ch]['l1'].wait_recv()
        dst = d2d.at[ch, xs[3], 1]
        merge_into(dst, [dst, step1.at[ch, 1]])
        rs[ch]['l2'] = remote(d2d.at[ch, xs[3]], step2.at[ch, 1], rs_send.at[ch, 7], rs_recv.at[ch, 7], left)
        rs[ch]['l2'].start()

    def project(ch):
        rs[ch]['r2'].wait_recv()
        rs[ch]['l2'].wait_recv()
        for kv in range(kv_local):
            mixed, _, total = merged([d2d.at[ch, xs[0], kv], step2.at[ch, 0, kv], step2.at[ch, 1, kv]])
            heads = (mixed / total).T.astype(BF16)
            for g in range(group):
                col = (kv * group + g) * head_dim
                heads_ref[:, col:col + head_dim] = heads[g * toks:(g + 1) * toks]
        if ch == 0:
            w_copy.wait()
        tile = width // 10

        @pl.loop(0, 10)
        def _(n):
            at = pl.ds(pl.multiple_of(n * tile, tile), tile)
            product = jnp.dot(heads_ref[...], w_ref[:, at], preferred_element_type=F32).astype(BF16).astype(F32)
            for d in range(ny):
                part[ch, d, :, at] = product[d * rows:(d + 1) * rows]

        low, high = pl.ds(0, half), pl.ds(half, half)
        rs[ch]['u1'] = remote(part.at[ch, ys[2], :, low], tp1.at[ch, 0], rs_send.at[ch, 8], rs_recv.at[ch, 8], up)
        rs[ch]['d1'] = remote(part.at[ch, ys[2], :, high], tp1.at[ch, 1], rs_send.at[ch, 9], rs_recv.at[ch, 9], down)
        rs[ch]['u1'].start()
        rs[ch]['d1'].start()

    def tp_step(ch):
        rs[ch]['u1'].wait_recv()
        part[ch, ys[1], :, :half] += tp1[ch, 0]
        rs[ch]['u2'] = remote(part.at[ch, ys[1]], tp2.at[ch, 0], rs_send.at[ch, 10], rs_recv.at[ch, 10], up)
        rs[ch]['u2'].start()
        rs[ch]['d1'].wait_recv()
        part[ch, ys[3], :, half:] += tp1[ch, 1]
        rs[ch]['d2'] = remote(part.at[ch, ys[3]], tp2.at[ch, 1], rs_send.at[ch, 11], rs_recv.at[ch, 11], down)
        rs[ch]['d2'].start()

    sends = []
    recvs = [dict() for _ in range(num_chunks)]
    q_all = (0, 4)
    q_a, q_b = (0, 2), (2, 2)

    def piece(ch, dx, dy, q):
        return full.at[ch, xs[dx], core, ys[dy], :, pl.ds(q[0] * quarter, q[1] * quarter)]

    used = [0] * num_chunks

    def hop(ch, dx, dy, q, peer, tag):
        n = used[ch]
        used[ch] += 1
        src = piece(ch, dx, dy, q)
        copy = remote(src, src, ag_send.at[ch, n], ag_recv.at[ch, n], peer)
        copy.start()
        sends.append(copy)
        recvs[ch][tag] = copy

    def pair_block(ch, dx, dy):
        n = dx * ny + dy
        src = full.at[ch, xs[dx], core, ys[dy]]
        copy = remote(src, src, pr_send.at[ch, n], pr_recv.at[ch, n], partner)
        copy.start()
        sends.append(copy)
        recvs[ch]['pair', dx, dy] = copy

    def finish(ch):
        x_copies[ch].wait()
        rs[ch]['u2'].wait_recv()
        rs[ch]['d2'].wait_recv()
        summed = part[ch, ys[0]] + tp2[ch, 0] + tp2[ch, 1]
        full[ch, xs[0], core, ys[0]] = (xres[ch].astype(F32) + summed).astype(BF16).astype(F32)
        hop(ch, 0, 0, q_all, right, 'R0')
        hop(ch, 0, 0, q_all, left, 'L0')
        hop(ch, 0, 0, q_all, up, 'U0')
        hop(ch, 0, 0, q_all, down, 'D0')
        pair_block(ch, 0, 0)

    def gather1(ch):
        got = recvs[ch]
        got['R0'].wait_recv()
        hop(ch, 3, 0, q_a, right, 'R1')
        hop(ch, 3, 0, q_a, up, 'U1m')
        hop(ch, 3, 0, q_a, down, 'D1m')
        got['L0'].wait_recv()
        hop(ch, 1, 0, q_b, left, 'L1')
        hop(ch, 1, 0, q_a, up, 'U1p')
        hop(ch, 1, 0, q_a, down, 'D1p')
        got['U0'].wait_recv()
        hop(ch, 0, 3, q_a, up, 'U1')
        hop(ch, 0, 3, q_b, right, 'R1m')
        hop(ch, 0, 3, q_b, left, 'L1m')
        got['D0'].wait_recv()
        hop(ch, 0, 1, q_b, down, 'D1')
        hop(ch, 0, 1, q_b, right, 'R1p')
        hop(ch, 0, 1, q_b, left, 'L1p')
        for dx, dy in ((3, 0), (1, 0), (0, 3), (0, 1)):
            pair_block(ch, dx, dy)

    def gather2(ch):
        got = recvs[ch]
        got['R1'].wait_recv()
        hop(ch, 2, 0, q_a, up, 'U2')
        hop(ch, 2, 0, q_a, down, 'D2')
        got['D1'].wait_recv()
        hop(ch, 0, 2, q_b, right, 'R2')
        hop(ch, 0, 2, q_b, left, 'L2')
        got['L1'].wait_recv()
        got['U1'].wait_recv()
        pair_block(ch, 2, 0)
        pair_block(ch, 0, 2)

    def gather3(ch):
        got = recvs[ch]
        got['U1m'].wait_recv()
        hop(ch, 3, 3, (0, 1), up, 'U3m')
        got['R1m'].wait_recv()
        hop(ch, 3, 3, (2, 1), right, 'R3m')
        pair_block(ch, 3, 3)
        got['D1m'].wait_recv()
        hop(ch, 3, 1, (1, 1), down, 'D3m')
        got['R1p'].wait_recv()
        hop(ch, 3, 1, (2, 1), right, 'R3p')
        pair_block(ch, 3, 1)
        got['U1p'].wait_recv()
        hop(ch, 1, 3, (0, 1), up, 'U3p')
        got['L1m'].wait_recv()
        hop(ch, 1, 3, (3, 1), left, 'L3m')
        pair_block(ch, 1, 3)
        got['D1p'].wait_recv()
        hop(ch, 1, 1, (1, 1), down, 'D3p')
        got['L1p'].wait_recv()
        hop(ch, 1, 1, (3, 1), left, 'L3p')
        pair_block(ch, 1, 1)
        got['U2'].wait_recv()
        hop(ch, 2, 3, (0, 1), up, 'U4')
        got['R2'].wait_recv()
        hop(ch, 3, 2, (2, 1), right, 'R4')
        got['D2'].wait_recv()
        hop(ch, 2, 1, (1, 1), down, 'D4')
        got['L2'].wait_recv()
        hop(ch, 1, 2, (3, 1), left, 'L4')

    def gather4(ch):
        got = recvs[ch]
        got['U3m'].wait_recv()
        got['D3m'].wait_recv()
        pair_block(ch, 3, 2)
        got['U3p'].wait_recv()
        got['D3p'].wait_recv()
        pair_block(ch, 1, 2)
        got['R3m'].wait_recv()
        got['L3m'].wait_recv()
        pair_block(ch, 2, 3)
        got['R3p'].wait_recv()
        got['L3p'].wait_recv()
        pair_block(ch, 2, 1)
        for tag in ('U4', 'R4', 'D4', 'L4'):
            got[tag].wait_recv()
        pair_block(ch, 2, 2)

    outs = []

    def emit(ch):
        for dx in range(nx):
            for dy in range(ny):
                recvs[ch]['pair', dx, dy].wait_recv()

        @pl.loop(0, nx * 2)
        def _(n):
            for d in range(ny):
                stage[ch, n, d * rows:(d + 1) * rows] = full[ch, n // 2, n % 2, d].astype(BF16)

        per = nx * 2
        copy = pltpu.make_async_copy(stage.at[ch], y_hbm.at[pl.ds(ch * per, per)], out_sem.at[ch])
        copy.start()
        outs.append(copy)

    steps = (cp_pair, cp_step, project, tp_step, finish, gather1, gather2, gather3, gather4, emit)
    lag = 1
    for tick in range(len(steps) + lag * (num_chunks - 1)):
        for ch in range(num_chunks):
            if 0 <= tick - lag * ch < len(steps):
                steps[tick - lag * ch](ch)
    for ch in range(num_chunks):
        for copy in rs[ch].values():
            copy.wait_send()
    for copy in sends:
        copy.wait_send()
    for copy in outs:
        copy.wait()


def combine(num_chunks, nx, ny, partial, hidden, w_out, head_dim):
    num_reqs, halves, kv_local, depth, lanes = partial.shape
    total_rows, width = hidden.shape[0] * hidden.shape[1], hidden.shape[2]
    toks = total_rows // (num_chunks * nx * 2)
    rows = toks // ny
    feats = w_out.shape[0]
    a = partial.reshape(num_chunks, nx, 2, kv_local, depth, lanes)
    hid = hidden.reshape(num_chunks * nx * 2 * ny, rows, width)
    scale = head_dim ** -0.5 * math.log2(math.e)
    dma = pltpu.SemaphoreType.DMA
    out = pl.pallas_call(
        functools.partial(combine_kernel, num_chunks, nx, ny, scale),
        in_specs=[pl.BlockSpec(memory_space=pltpu.VMEM), pl.BlockSpec(memory_space=pl.ANY), pl.BlockSpec(memory_space=pl.ANY)],
        out_specs=pl.BlockSpec(memory_space=pl.ANY),
        out_shape=jax.ShapeDtypeStruct((num_chunks * nx * 2, toks, width), BF16),
        scratch_shapes=[
            pltpu.VMEM((feats, width), BF16),
            pltpu.VMEM((num_chunks, rows, width), BF16),
            pltpu.VMEM((num_chunks, nx, kv_local, depth, lanes), F32),
            pltpu.VMEM((num_chunks, 2, depth, lanes), F32),
            pltpu.VMEM((num_chunks, 2, kv_local, depth, lanes), F32),
            pltpu.VMEM((toks, feats), BF16),
            pltpu.VMEM((num_chunks, ny, rows, width), F32),
            pltpu.VMEM((num_chunks, 2, rows, width // 2), F32),
            pltpu.VMEM((num_chunks, 2, rows, width), F32),
            pltpu.VMEM((num_chunks, nx, 2, ny, rows, width), F32),
            pltpu.VMEM((num_chunks, nx * 2, toks, width), BF16),
            dma, dma((num_chunks,)), dma((num_chunks,)),
            dma((num_chunks, 12)), dma((num_chunks, 12)),
            dma((num_chunks, 32)), dma((num_chunks, 32)),
            dma((num_chunks, nx * ny)), dma((num_chunks, nx * ny)),
        ],
        compiler_params=pltpu.CompilerParams(collective_id=0, has_side_effects=True, vmem_limit_bytes=60 * 1024 * 1024),
        name="combine",
    )(a, hid, w_out)
    return out.reshape(hidden.shape)


def solution(mesh):
    cp_size, tp_size = mesh.shape['cp'], mesh.shape['tp']
    cache_spec = P('dp', None, 'cp', 'tp')
    row_spec = P('dp')

    def local_step(hidden, attn_gain, w_query, w_key, w_value, w_out, cache_k, cache_v, ctx_len, positions, tree_mask):
        num_reqs, tree_len, width = hidden.shape
        head_dim = cache_k.shape[5]
        halves = max(1, NUM_CHUNKS * cp_size // num_reqs)
        cos_tab, sin_tab = rope_tables(positions, head_dim)
        q, kn, vn = project_qkv(hidden.reshape(num_reqs * tree_len, width), attn_gain[None, :], cos_tab, sin_tab, w_query, w_key, w_value)
        cp_rank = lax.axis_index('cp').astype(jnp.int32).reshape(1)
        partial, new_k, new_v = attend(cp_size, halves, ctx_len, cp_rank, q, kn, vn, tree_mask, cache_k, cache_v)
        out = combine(NUM_CHUNKS, cp_size // 2, tp_size, partial, hidden, w_out, head_dim)
        return out, new_k, new_v

    return jax.shard_map(local_step, mesh=mesh, in_specs=(row_spec, P(), P(None, 'tp'), P(None, 'tp'), P(None, 'tp'), P('tp', None), cache_spec, cache_spec, row_spec, row_spec, row_spec), out_specs=(row_spec, cache_spec, cache_spec), check_vma=False)
```
